32 devices in a mesh: dp: 1 (over z), vp: 32 (over y, x, core).
Axes of the slice: x: 4, y: 4, z: 1, core: 2. Of those that a mesh axis runs over, the one named last changes fastest.
The devices are a block of a 4x4x8 slice.
Arguments:
- hidden: bfloat16 [1024, 5120], P(('dp', 'vp'))
- target: int32 [1024], P('dp')
- norm_gain: bfloat16 [5120], replicated
- head_weight: bfloat16 [5120, 151936], P(None, 'vp')
Outputs:
- output 1: float32 [1024], P('dp')
- output 2: float32 [1024], P('dp')
- output 3: float32 [1], P('dp')
All inputs are finite; a program needn't handle non-finite values.
Results may differ from the reference program's by a relative error of at most 0.001.
Values are sent between devices in bfloat16 or wider.
A program may use at most 768 MiB of HBM per device.

```python
import math
import jax
import jax.numpy as jnp
from jax import lax

D = 5120
VOCAB = 151936
TOK_DEV = 32
GROUP = 32
HEAD_BLOCK = 128
NORM_EPS = 1e-6
TOKENS = TOK_DEV * GROUP
ROW_BLOCK = math.gcd(TOKENS, 64)


def setup_inputs(seed: int = 0, part: int = 0) -> dict:
    key = jax.random.key(seed)
    part_key = jax.random.fold_in(key, part)
    hidden_key, target_key = jax.random.split(part_key)
    gain_key, head_key = jax.random.split(jax.random.fold_in(key, 1000003))
    hidden = jax.random.normal(hidden_key, (TOKENS, D), jnp.float32).astype(jnp.bfloat16)
    target = jax.random.randint(target_key, (TOKENS,), 0, VOCAB, jnp.int32)
    target = target.at[0].set(0).at[TOKENS - 1].set(VOCAB - 1)
    norm_gain = (1.0 + 0.5 * jax.random.normal(gain_key, (D,), jnp.float32)).astype(jnp.bfloat16)
    head_scale = 1.5 / math.sqrt(D)

    def draw_rows(row_key):
        return (jax.random.normal(row_key, (HEAD_BLOCK, VOCAB), jnp.float32) * head_scale).astype(jnp.bfloat16)

    head_weight = lax.map(draw_rows, jax.random.split(head_key, D // HEAD_BLOCK)).reshape(D, VOCAB)
    return {"hidden": hidden, "target": target, "norm_gain": norm_gain, "head_weight": head_weight}


def reference(hidden, target, norm_gain, head_weight):
    hidden_f32 = hidden.astype(jnp.float32)
    inv_rms = lax.rsqrt(jnp.mean(hidden_f32 * hidden_f32, axis=-1, keepdims=True) + NORM_EPS)
    normed = (hidden_f32 * inv_rms * norm_gain.astype(jnp.float32)).astype(jnp.bfloat16)
    vocab_ids = jnp.arange(VOCAB, dtype=jnp.int32)

    def score_block(block_args):
        block_rows, block_target = block_args
        logits = jnp.dot(block_rows, head_weight, preferred_element_type=jnp.float32)
        row_max = jnp.max(logits, axis=-1, keepdims=True)
        shifted = logits - row_max
        exp_vals = jnp.exp(shifted)
        exp_total = jnp.sum(exp_vals, axis=-1)
        moment = jnp.sum(exp_vals * shifted, axis=-1)
        target_shift = jnp.sum(jnp.where(vocab_ids[None, :] == block_target[:, None], shifted, 0.0), axis=-1)
        log_total = jnp.log(exp_total)
        return target_shift - log_total, log_total - moment / exp_total

    num_blocks = TOKENS // ROW_BLOCK
    log_prob, entropy = lax.map(score_block, (normed.reshape(num_blocks, ROW_BLOCK, D), target.reshape(num_blocks, ROW_BLOCK)))
    log_prob = log_prob.reshape(TOKENS)
    entropy = entropy.reshape(TOKENS)
    return log_prob, entropy, jnp.mean(log_prob).reshape(1)
```

```python
import functools
import math

import jax
import jax.numpy as jnp
from jax import lax
from jax.experimental import pallas as pl
from jax.experimental.pallas import tpu as pltpu
from jax.sharding import PartitionSpec as P

NORM_EPS = 1e-6
TILE = 256
LANES = 128
STEP = 528
PIECE = 88
SEGMENTS = 3
FLOOR = -200.0


def _chunks(vocab):
    units = -(-vocab // 16)
    count = -(-units * 16 // STEP)
    ends = [units * (i + 1) // count * 16 for i in range(count)]
    return [(start, end - start) for start, end in zip([0] + ends, ends)]


def _kernel(
    side, hid_hbm, tgt_hbm, rest_hbm, w_hbm, lp_ref, ent_ref, mean_ref,
    hid, tgt, w, h, ids, local_ids, ms, zs, ss, ts, stat, hold, recv, zbuf,
    in_sem, w_sem, s_send, s_recv, st_send, st_recv,
):
    n = 2 * side * side
    rows, depth = hid.shape
    vocab = w_hbm.shape[0]
    ktiles = depth // TILE
    group = rows * side
    me = lax.axis_index("vp")
    core = lax.rem(me, 2)
    x = lax.rem(me // 2, side)
    y = me // (2 * side)
    first = jnp.where(core == 0, x, y)
    second = jnp.where(core == 0, y, x)
    partner = me + 1 - 2 * core

    def device(p1, p2):
        return jnp.where(core == 0, (p2 * side + p1) * 2, (p1 * side + p2) * 2 + 1)

    def turn(p, by):
        return lax.rem(p + by + side, side)

    def group_row(kind, p2):
        return (kind * side + p2) * group

    whole = vocab // 16 * 16
    small = [
        pltpu.make_async_copy(src, dst, in_sem.at[i])
        for i, (src, dst) in enumerate(((hid_hbm, hid), (rest_hbm, w.at[pl.ds(whole, 16), :]), (tgt_hbm, tgt)))
    ]
    for c in small:
        c.start()
    chunks = _chunks(vocab)
    per = -(-len(chunks) // SEGMENTS)
    cuts = [chunks[i][0] for i in range(0, len(chunks), per)] + [whole]

    def head_copy(i):
        at = pl.ds(cuts[i], cuts[i + 1] - cuts[i])
        return pltpu.make_async_copy(w_hbm.at[at, :], w.at[at, :], w_sem.at[i])

    for i in range(len(cuts) - 1):
        head_copy(i).start()

    barrier = pltpu.get_barrier_semaphore()

    def greet(k, _):
        pl.semaphore_signal(barrier, inc=1, device_id={"vp": lax.rem(me + k, n)}, device_id_type=pl.DeviceIdType.MESH)
        return 0

    lax.fori_loop(1, n, greet, 0)

    small[0].wait()
    small[1].wait()
    xf = hid[...].astype(jnp.float32)
    inv = lax.rsqrt(jnp.mean(xf * xf, axis=-1, keepdims=True) + NORM_EPS)
    own = pl.multiple_of(group_row(core, second) + first * rows, rows)
    gain = w[whole : whole + 16, :].astype(jnp.float32)[vocab - whole : vocab - whole + 1]
    h[pl.ds(own, rows), :] = (xf * inv * gain).astype(jnp.bfloat16)

    def send(slot, row, count, to):
        at = h.at[pl.ds(pl.multiple_of(row, 16), count), :]
        return pltpu.make_async_remote_copy(
            src_ref=at, dst_ref=at, send_sem=s_send.at[slot], recv_sem=s_recv.at[slot],
            device_id={"vp": to}, device_id_type=pl.DeviceIdType.MESH,
        )

    half = rows // 2
    next1, prev1, far1 = turn(first, 1), turn(first, -1), turn(first, 2)
    next2, prev2, far2 = turn(second, 1), turn(second, -1), turn(second, 2)
    up1, down1 = device(next1, second), device(prev1, second)
    up2, down2 = device(first, next2), device(first, prev2)
    base = group_row(core, second)
    below, above, across = base + prev1 * rows, base + next1 * rows, base + far1 * rows
    pair = 2 * rows
    mine, lower, upper, opposite = (group_row(core, p) for p in (second, prev2, next2, far2))

    pl.semaphore_wait(barrier, n - 1)
    sends = [
        send(0, own, half, up1),
        send(1, own + half, half, down1),
        send(2, own + half, half, up1),
        send(3, own, half, down1),
        send(4, own, rows, partner),
    ]
    for c in sends:
        c.start()
    arrive = lambda slot, count: send(slot, 0, count, partner).wait_recv()

    small[2].wait()
    lane1 = lax.broadcasted_iota(jnp.int32, (1, LANES), 1)
    part = lane1 // rows
    turned = [tgt[...]] + [pltpu.roll(tgt[...], i * rows, 1) for i in range(1, side)]

    def by_part(pieces):
        out = pieces[-1]
        for i in range(len(pieces) - 2, -1, -1):
            out = jnp.where(part == i, pieces[i], out)
        return out

    def cut(arrays, row, move):
        return arrays[move % side][row : row + 1]

    for g in range(side):
        ids[g : g + 1, :] = by_part([cut(turned, 2 * g + i // 2, i - i % 2 * 2) for i in range(side)])
        ids[side + g : side + g + 1, :] = by_part(
            [cut(turned, 2 * i + g // 2, i - g % 2 * 2 - 1) for i in range(side)]
        )

    arrive(0, half)
    sends.append(send(5, below, half, up1))
    sends[-1].start()
    arrive(1, half)
    sends.append(send(6, above + half, half, down1))
    sends[-1].start()
    arrive(2, half)
    arrive(3, half)
    sends += [send(7, below, rows, partner), send(8, above, rows, partner)]
    sends[-2].start()
    sends[-1].start()
    arrive(5, half)
    arrive(6, half)
    sends.append(send(9, across, rows, partner))
    sends[-1].start()
    later = [
        send(10, mine, pair, up2),
        send(11, mine + pair, pair, down2),
        send(12, mine + pair, pair, up2),
        send(13, mine, pair, down2),
    ]
    for c in later:
        c.start()
    sends += later

    forward = [send(14, lower, pair, up2), send(15, upper + pair, pair, down2)]
    share1 = [send(16, lower, pair, partner), send(17, upper + pair, pair, partner)]
    share2 = [send(18, lower + pair, pair, partner), send(19, upper, pair, partner)]
    share3 = [send(20, opposite, pair, partner), send(21, opposite + pair, pair, partner)]
    sends += forward + share1 + share2 + share3

    def pass_on(arrivals, copies):
        for slot in arrivals:
            arrive(slot, pair)
        for c in copies:
            c.start()

    def stat_copy(slot, count, to):
        return pltpu.make_async_remote_copy(
            src_ref=stat.at[pl.ds(slot, count)], dst_ref=recv.at[pl.ds(slot, count), me],
            send_sem=st_send, recv_sem=st_recv,
            device_id={"vp": to}, device_id_type=pl.DeviceIdType.MESH,
        )

    def spread(slot, count):
        def one(k, _):
            stat_copy(slot, count, lax.rem(me + k, n)).start()
            return 0

        lax.fori_loop(1, n, one, 0)

    lane = lax.broadcasted_iota(jnp.int32, (8, LANES), 1)
    sub = lax.broadcasted_iota(jnp.int32, (8, LANES), 0)

    def update(kind, row, tiles, keep=None):
        at = pl.ds(kind * LANES, LANES)
        last = len(tiles) - 1
        if keep is not None:
            tiles[last] = jnp.where(keep, tiles[last], -jnp.inf)
        old = ms[:, at]
        level = list(tiles)
        while len(level) > 1:
            level = [jnp.maximum(*level[i : i + 2]) if i + 1 < len(level) else level[i] for i in range(0, len(level), 2)]
        top = jnp.maximum(old, level[0])
        down = jnp.maximum(old - top, FLOOR)
        scale = jnp.exp(down)
        z, t = zs[:, at], ts[:, at]
        s = scale * (ss[:, at] + z * down)
        z = scale * z
        local = local_ids[kind]
        for i, v in enumerate(tiles):
            d = v - top
            hit = local == row + 8 * i
            if keep is not None and i == last:
                d = jnp.maximum(d, FLOOR)
                hit = jnp.logical_and(hit, keep)
            e = jnp.exp(d)
            z = z + e
            s = s + e * d
            t = jnp.where(hit, v, t)
        ms[:, at], zs[:, at], ss[:, at], ts[:, at] = top, z, s, t

    def reset(lo, hi):
        ms[...] = jnp.full(ms.shape, -jnp.inf, jnp.float32)
        for r in (zs, ss, ts):
            r[...] = jnp.zeros(r.shape, jnp.float32)
        for kind, place in ((0, y), (1, x)):
            a = ids[pl.ds(kind * side + turn(place, lo), 1), :]
            b = ids[pl.ds(kind * side + turn(place, hi), 1), :]
            wanted = jnp.where(lane1 < pair, a, b) - me * vocab
            local_ids[kind] = jnp.broadcast_to(wanted, (8, LANES)) - sub

    def close():
        out = []
        for kind in range(2):
            at = pl.ds(kind * LANES, LANES)
            m, z = ms[:, at], zs[:, at]
            top = jnp.max(m, axis=0, keepdims=True)
            down = jnp.maximum(m - top, FLOOR)
            scale = jnp.exp(down)
            out += [
                top,
                jnp.sum(scale * z, axis=0, keepdims=True),
                jnp.sum(scale * (ss[:, at] + z * down), axis=0, keepdims=True),
                jnp.sum(ts[:, at], axis=0, keepdims=True),
            ]
        return jnp.concatenate(out, axis=0)

    def block_work(accs, b):
        lo = jnp.where(b == 0, 0, jnp.where(b == 1, -1, jnp.where(b == 2, 1, 2)))
        hi = jnp.where(b == 0, 0, jnp.where(b == 1, 1, jnp.where(b == 2, -1, 2)))
        offsets = []
        for kind, place in ((0, y), (1, x)):
            offsets.append(pl.multiple_of(group_row(kind, turn(place, lo)), pair))
            offsets.append(pl.multiple_of(group_row(kind, turn(place, hi)) + pair, pair))

        @pl.when(b == 0)
        def _():
            for slot in (4, 7, 8, 9):
                arrive(slot, rows)

        for j in range(1, 4):

            @pl.when(b == j)
            def _():
                arrive(14 + 2 * j, pair)
                arrive(15 + 2 * j, pair)

        reset(lo, hi)

        def tokens(k):
            return jnp.concatenate([h[pl.ds(o, pair), k * TILE : (k + 1) * TILE] for o in offsets], axis=0)

        def product(c):
            start, count = chunks[c]
            rhs = jnp.concatenate([h[pl.ds(o, pair), :] for o in offsets], axis=0)
            return lax.dot_general(
                w[start : start + count, :], rhs, (((1,), (1,)), ((), ())), preferred_element_type=jnp.float32
            )

        def statistics(c, z):
            start, count = chunks[c]
            for r in range(0, count, PIECE):
                for kind in range(2):
                    tiles = [z[r + j : r + j + 8, kind * LANES : (kind + 1) * LANES] for j in range(0, min(PIECE, count - r), 8)]
                    edge = start + r + 8 * len(tiles)
                    keep = sub < vocab - edge + 8 if edge > vocab else None
                    update(kind, start + r, tiles, keep)

        for c in range(len(chunks)):
            if c % per == 0:

                @pl.when(b == 0)
                def _():
                    head_copy(c // per).wait()

            if c == 2 * per:

                @pl.when(b == 0)
                def _():
                    pass_on((10, 11), forward + share1)

            if c == per:

                @pl.when(b == 1)
                def _():
                    pass_on((12, 13), share2)

                @pl.when(b == 2)
                def _():
                    pass_on((14, 15), share3)

            zbuf[c % 2, : chunks[c][1]] = product(c)
            if c:
                statistics(c - 1, zbuf.at[(c - 1) % 2])
        statistics(len(chunks) - 1, zbuf.at[(len(chunks) - 1) % 2])
        finish(b)

        return 0

    def finish(b):
        p = close()

        def put(slot, v):
            stat[slot] = v
            recv[slot, me] = v

        @pl.when(b == 0)
        def _():
            put(0, p)
            spread(0, 1)

        @pl.when(b == 1)
        def _():
            hold[...] = p

        @pl.when(b == 2)
        def _():
            q = hold[...]
            put(1, jnp.where(lane < pair, q, p))
            put(2, jnp.where(lane < pair, p, q))
            spread(1, 2)

        @pl.when(b == 3)
        def _():
            put(3, p)
            spread(3, 1)

    def one_block(b, _):
        return block_work(None, b)

    lax.fori_loop(0, 4, one_block, 0)

    for c in sends:
        c.wait_send()
    everything = recv.at[:, pl.ds(0, n - 1)]
    pltpu.make_async_copy(everything, everything, st_recv).wait()
    pltpu.make_async_copy(everything, everything, st_send).wait()

    slot_of = {0: 0, side - 1: 1, 1: 2, 2: 3}
    low = sub < 4
    q4 = lax.rem(sub, 4)
    lps, ents = [None] * (2 * side), [None] * (2 * side)
    for g in range(side):

        def value(d):
            dx, dy = (d // 2) % side, d // (2 * side)
            a = recv[slot_of[(g - dy) % side], d]
            b = recv[slot_of[(g - dx) % side], d]
            return jnp.where(low, a, b)

        top = functools.reduce(jnp.maximum, [value(d) for d in range(n)])
        total = jnp.zeros((8, LANES), jnp.float32)
        for d in range(n):
            v = value(d)
            gap = v - top
            down = jnp.where(low, jnp.broadcast_to(gap[0:1, :], (8, LANES)), jnp.broadcast_to(gap[4:5, :], (8, LANES)))
            down = jnp.maximum(down, FLOOR)
            scaled = v * jnp.exp(down)
            moved = pltpu.roll(scaled * down, 1, 0)
            total = total + jnp.where(q4 == 3, v, scaled) + jnp.where(q4 == 2, moved, 0.0)
        for k in range(2):
            m, z, s, t = top[4 * k : 4 * k + 1], *(total[4 * k + i : 4 * k + i + 1] for i in (1, 2, 3))
            log_z = jnp.log(z)
            lps[k * side + g] = (t - m) - log_z
            ents[k * side + g] = log_z - s / z

    for parts, ref in ((lps, lp_ref), (ents, ent_ref)):
        both = jnp.concatenate(parts, axis=0)
        moved = [both] + [pltpu.roll(both, i * rows, 1) for i in range(1, side)]
        for r in range(2 * side):
            q, hx = r // 2, r % 2
            ref[r : r + 1, :] = by_part(
                [
                    cut(moved, q, -2 * hx),
                    cut(moved, side + 2 * hx, 1 - q),
                    cut(moved, q, 1 - 2 * hx),
                    cut(moved, side + 2 * hx + 1, 3 - q),
                ]
            )
    mean_ref[0] = jnp.sum(lp_ref[...]) / (2 * side * group)


def solution(mesh):
    n = mesh.shape["vp"]
    side = math.isqrt(n // 2)

    def local_step(hidden, target, norm_gain, head_weight):
        rows, depth = hidden.shape
        tokens = target.shape[0]
        group = rows * side
        vocab = head_weight.shape[1]
        whole = vocab // 16 * 16
        rest = jnp.concatenate([head_weight.T[whole:], norm_gain[None]])
        rest = jnp.pad(rest, ((0, 16 - rest.shape[0]), (0, 0)))
        lp, entropy, mean = pl.pallas_call(
            functools.partial(_kernel, side),
            out_shape=(
                jax.ShapeDtypeStruct((2 * side, group), jnp.float32),
                jax.ShapeDtypeStruct((2 * side, group), jnp.float32),
                jax.ShapeDtypeStruct((1,), jnp.float32),
            ),
            in_specs=[pl.BlockSpec(memory_space=pl.ANY)] * 4,
            out_specs=(
                pl.BlockSpec(memory_space=pltpu.VMEM),
                pl.BlockSpec(memory_space=pltpu.VMEM),
                pl.BlockSpec(memory_space=pltpu.SMEM),
            ),
            scratch_shapes=[
                pltpu.VMEM((rows, depth), jnp.bfloat16),
                pltpu.VMEM((2 * side, group), jnp.int32),
                pltpu.VMEM((whole + 16, depth), jnp.bfloat16),
                pltpu.VMEM((tokens, depth), jnp.bfloat16),
                pltpu.VMEM((2 * side, group), jnp.int32),
                pltpu.VMEM((2, 8, LANES), jnp.int32),
                *[pltpu.VMEM((8, 2 * LANES), jnp.float32)] * 4,
                pltpu.VMEM((side, 8, LANES), jnp.float32),
                pltpu.VMEM((8, LANES), jnp.float32),
                pltpu.VMEM((side, n, 8, LANES), jnp.float32),
                pltpu.VMEM((2, STEP, TILE), jnp.float32),
                pltpu.SemaphoreType.DMA((3,)),
                pltpu.SemaphoreType.DMA((SEGMENTS,)),
                pltpu.SemaphoreType.DMA((22,)),
                pltpu.SemaphoreType.DMA((22,)),
                pltpu.SemaphoreType.DMA,
                pltpu.SemaphoreType.DMA,
            ],
            compiler_params=pltpu.CompilerParams(
                collective_id=0, has_side_effects=True, vmem_limit_bytes=67043328
            ),
            name="score",
        )(hidden, target.reshape(2 * side, group), rest, head_weight.T)
        return lp.reshape(tokens), entropy.reshape(tokens), mean

    return jax.shard_map(
        local_step,
        mesh=mesh,
        in_specs=(P(("dp", "vp"), None), P("dp"), P(None), P(None, "vp")),
        out_specs=(P("dp"), P("dp"), P("dp")),
        check_vma=False,
    )
```

```python
import functools
import math

import jax
import jax.numpy as jnp
from jax import lax
from jax.experimental import pallas as pl
from jax.experimental.pallas import tpu as pltpu
from jax.sharding import PartitionSpec as P

NORM_EPS = 1e-6
TILE = 256
LANES = 128
PIECE = 80
SEGMENTS = 3
PAIRS = 2
FLOOR = -200.0


def _chunks(vocab):
    units = -(-vocab // 16)
    count = SEGMENTS * PAIRS
    size = -(-units // (2 * count)) * 2
    out, start = [], 0
    for _ in range(count):
        both = min(size, units - start)
        for rows in (both - both // 2, both // 2):
            out.append((start * 16, rows * 16))
            start += rows
    return out


def _kernel(
    side, hid_hbm, tgt_hbm, gain_hbm, rest_hbm, w_hbm, parts_ref, mean_ref,
    hid, tgt, gain, w, h, ids, local_ids, ms, zs, ss, ts, stat, hold, recv, zbuf,
    in_sem, w_sem, s_send, s_recv, st_send, st_recv,
):
    n = 2 * side * side
    rows, depth = hid.shape
    vocab = w_hbm.shape[0]
    ktiles = depth // TILE
    group = rows * side
    me = lax.axis_index("vp")
    core = lax.rem(me, 2)
    x = lax.rem(me // 2, side)
    y = me // (2 * side)
    first = jnp.where(core == 0, x, y)
    second = jnp.where(core == 0, y, x)
    partner = me + 1 - 2 * core

    def device(p1, p2):
        return jnp.where(core == 0, (p2 * side + p1) * 2, (p1 * side + p2) * 2 + 1)

    def turn(p, by):
        return lax.rem(p + by + side, side)

    def group_row(kind, p2):
        return (kind * side + p2) * group

    half = rows // 2
    next1, prev1, far1 = turn(first, 1), turn(first, -1), turn(first, 2)
    next2, prev2, far2 = turn(second, 1), turn(second, -1), turn(second, 2)
    up1, down1 = device(next1, second), device(prev1, second)
    up2, down2 = device(first, next2), device(first, prev2)

    near = (partner, up1, down1, up2, down2)
    barrier = pltpu.get_barrier_semaphore()
    for to in near:
        pl.semaphore_signal(barrier, inc=1, device_id={"vp": to}, device_id_type=pl.DeviceIdType.MESH)

    whole = vocab // 16 * 16
    twice = 16 - vocab % 16
    small = [
        pltpu.make_async_copy(src, dst, in_sem.at[i])
        for i, (src, dst) in enumerate(
            ((hid_hbm, hid), (gain_hbm, gain), (tgt_hbm, tgt), (rest_hbm, w.at[pl.ds(whole, 16), :]))
        )
    ]
    for c in small:
        c.start()
    chunks = _chunks(vocab)
    per = 2 * PAIRS
    cuts = [chunks[i][0] for i in range(0, len(chunks), per)] + [whole]

    def head_copy(i):
        at = pl.ds(cuts[i], cuts[i + 1] - cuts[i])
        return pltpu.make_async_copy(w_hbm.at[at, :], w.at[at, :], w_sem.at[i])

    for i in range(len(cuts) - 1):
        head_copy(i).start(priority=1)

    small[0].wait()
    small[1].wait()
    xf = hid[...].astype(jnp.float32)
    inv = lax.rsqrt(jnp.mean(xf * xf, axis=-1, keepdims=True) + NORM_EPS)
    own = pl.multiple_of(group_row(core, second) + first * rows, rows)
    for i in range(depth // LANES):
        cols = slice(i * LANES, (i + 1) * LANES)
        part = xf[:, cols] * inv * gain[i : i + 1, :].astype(jnp.float32)
        h[pl.ds(own, rows), cols] = part.astype(jnp.bfloat16)

    def send(slot, row, count, to):
        at = h.at[pl.ds(pl.multiple_of(row, 16), count), :]
        return pltpu.make_async_remote_copy(
            src_ref=at, dst_ref=at, send_sem=s_send.at[slot], recv_sem=s_recv.at[slot],
            device_id={"vp": to}, device_id_type=pl.DeviceIdType.MESH,
        )

    base = group_row(core, second)
    below, above, across = base + prev1 * rows, base + next1 * rows, base + far1 * rows
    pair = 2 * rows
    mine, lower, upper, opposite = (group_row(core, p) for p in (second, prev2, next2, far2))

    pl.semaphore_wait(barrier, len(near))
    sends = [
        send(0, own, half, up1),
        send(1, own + half, half, down1),
        send(2, own + half, half, up1),
        send(3, own, half, down1),
        send(4, own, rows, partner),
    ]
    for c in sends:
        c.start()
    arrive = lambda slot, count: send(slot, 0, count, partner).wait_recv()

    small[2].wait()
    lane1 = lax.broadcasted_iota(jnp.int32, (1, LANES), 1)
    part = lane1 // rows
    turned = [tgt[...]] + [pltpu.roll(tgt[...], i * rows, 1) for i in range(1, side)]

    def by_part(pieces):
        out = pieces[-1]
        for i in range(len(pieces) - 2, -1, -1):
            out = jnp.where(part == i, pieces[i], out)
        return out

    def cut(arrays, row, move):
        return arrays[move % side][row : row + 1]

    for g in range(side):
        ids[g : g + 1, :] = by_part([cut(turned, 2 * g + i // 2, i - i % 2 * 2) for i in range(side)])
        ids[side + g : side + g + 1, :] = by_part(
            [cut(turned, 2 * i + g // 2, i - g % 2 * 2 - 1) for i in range(side)]
        )

    arrive(0, half)
    sends.append(send(5, below, half, up1))
    sends[-1].start()
    arrive(1, half)
    sends.append(send(6, above + half, half, down1))
    sends[-1].start()
    arrive(2, half)
    arrive(3, half)
    sends += [send(7, below, rows, partner), send(8, above, rows, partner)]
    sends[-2].start()
    sends[-1].start()
    arrive(5, half)
    arrive(6, half)
    sends.append(send(9, across, rows, partner))
    sends[-1].start()
    later = [
        send(10, mine, pair, up2),
        send(11, mine + pair, pair, down2),
        send(12, mine + pair, pair, up2),
        send(13, mine, pair, down2),
    ]
    for c in later:
        c.start()
    sends += later

    forward = [send(14, lower, pair, up2), send(15, upper + pair, pair, down2)]
    share1 = [send(16, lower, pair, partner), send(17, upper + pair, pair, partner)]
    share2 = [send(18, lower + pair, pair, partner), send(19, upper, pair, partner)]
    share3 = [send(20, opposite, pair, partner), send(21, opposite + pair, pair, partner)]
    sends += forward + share1 + share2 + share3

    def pass_on(arrivals, copies):
        for slot in arrivals:
            arrive(slot, pair)
        for c in copies:
            c.start()

    def stat_copy(slot, count, to):
        return pltpu.make_async_remote_copy(
            src_ref=stat.at[pl.ds(slot, count)], dst_ref=recv.at[pl.ds(slot, count), me],
            send_sem=st_send, recv_sem=st_recv,
            device_id={"vp": to}, device_id_type=pl.DeviceIdType.MESH,
        )

    def spread(slot, count):
        for k in range(1, n):
            stat_copy(slot, count, lax.rem(me + k, n)).start()

    lane = lax.broadcasted_iota(jnp.int32, (8, LANES), 1)
    sub = lax.broadcasted_iota(jnp.int32, (8, LANES), 0)

    def update(kind, tiles):
        at = pl.ds(kind * LANES, LANES)
        old = ms[:, at]
        level = [v if keep is None else jnp.where(keep, v, -jnp.inf) for _, keep, v in tiles]
        while len(level) > 1:
            level = [jnp.maximum(*level[i : i + 2]) if i + 1 < len(level) else level[i] for i in range(0, len(level), 2)]
        top = jnp.maximum(old, level[0])
        down = jnp.maximum(old - top, FLOOR)
        scale = jnp.exp(down)
        z, t = zs[:, at], ts[:, at]
        s = scale * (ss[:, at] + z * down)
        z = scale * z
        local = local_ids[kind]
        for row, keep, v in tiles:
            d = v - top
            hit = local == row
            if keep is not None:
                d = jnp.where(keep, d, FLOOR)
                hit = jnp.logical_and(hit, keep)
            e = jnp.exp(d)
            z = z + e
            s = s + e * d
            t = jnp.where(hit, v, t)
        ms[:, at], zs[:, at], ss[:, at], ts[:, at] = top, z, s, t

    def reset(lo, hi):
        ms[...] = jnp.full(ms.shape, -jnp.inf, jnp.float32)
        for r in (zs, ss, ts):
            r[...] = jnp.zeros(r.shape, jnp.float32)
        for kind, place in ((0, y), (1, x)):
            a = ids[pl.ds(kind * side + turn(place, lo), 1), :]
            b = ids[pl.ds(kind * side + turn(place, hi), 1), :]
            wanted = jnp.where(lane1 < pair, a, b) - me * vocab
            local_ids[kind] = jnp.broadcast_to(wanted, (8, LANES)) - sub

    def close():
        out = []
        for kind in range(2):
            at = pl.ds(kind * LANES, LANES)
            m, z = ms[:, at], zs[:, at]
            top = jnp.max(m, axis=0, keepdims=True)
            down = jnp.maximum(m - top, FLOOR)
            scale = jnp.exp(down)
            out += [
                top,
                jnp.sum(scale * z, axis=0, keepdims=True),
                jnp.sum(scale * (ss[:, at] + z * down), axis=0, keepdims=True),
                jnp.sum(ts[:, at], axis=0, keepdims=True),
            ]
        return jnp.concatenate(out, axis=0)

    def block_work(accs, b):
        lo = jnp.where(b == 0, 0, jnp.where(b == 1, -1, jnp.where(b == 2, 1, 2)))
        hi = jnp.where(b == 0, 0, jnp.where(b == 1, 1, jnp.where(b == 2, -1, 2)))
        offsets = []
        for kind, place in ((0, y), (1, x)):
            offsets.append(pl.multiple_of(group_row(kind, turn(place, lo)), pair))
            offsets.append(pl.multiple_of(group_row(kind, turn(place, hi)) + pair, pair))

        @pl.when(b == 0)
        def _():
            for slot in (4, 7, 8, 9):
                arrive(slot, rows)

        for j in range(1, 4):

            @pl.when(b == j)
            def _():
                arrive(14 + 2 * j, pair)
                arrive(15 + 2 * j, pair)
                if j == 3:
                    spread(0, 3)

        reset(lo, hi)

        def tokens(k):
            return jnp.concatenate([h[pl.ds(o, pair), k * TILE : (k + 1) * TILE] for o in offsets], axis=0)

        def product(c):
            start, count = chunks[c]
            rhs = jnp.concatenate([h[pl.ds(o, pair), :] for o in offsets], axis=0)
            return lax.dot_general(
                w[start : start + count, :], rhs, (((1,), (1,)), ((), ())), preferred_element_type=jnp.float32
            )

        def statistics(c, z):
            start, count = chunks[c]
            for r in range(0, count, PIECE):
                for kind in range(2):
                    tiles = []
                    for j in range(r, min(r + PIECE, count), 8):
                        row, keep = start + j, None
                        if row >= whole:
                            keep = sub >= twice - (row - whole)
                            row -= twice
                        tiles.append((row, keep, z[j : j + 8, kind * LANES : (kind + 1) * LANES]))
                    update(kind, tiles)

        for c in range(len(chunks)):
            if c % per == 0:

                @pl.when(b == 0)
                def _():
                    head_copy(c // per).wait()
                    if c == 2 * per:
                        small[3].wait()

            if c == 2 * per:

                @pl.when(b == 0)
                def _():
                    pass_on((10, 11), forward + share1)

            if c == per:

                @pl.when(b == 1)
                def _():
                    pass_on((12, 13), share2)

                @pl.when(b == 2)
                def _():
                    pass_on((14, 15), share3)

            zbuf[c % 2, : chunks[c][1]] = product(c)
            if c:
                statistics(c - 1, zbuf.at[(c - 1) % 2])
        statistics(len(chunks) - 1, zbuf.at[(len(chunks) - 1) % 2])
        finish(b)

        return 0

    def finish(b):
        p = close()

        def put(slot, v):
            stat[slot] = v
            recv[slot, me] = v

        @pl.when(b == 0)
        def _():
            put(0, p)

        @pl.when(b == 1)
        def _():
            hold[...] = p

        @pl.when(b == 2)
        def _():
            q = hold[...]
            put(1, jnp.where(lane < pair, q, p))
            put(2, jnp.where(lane < pair, p, q))

        @pl.when(b == 3)
        def _():
            put(3, p)
            spread(3, 1)

    def one_block(b, _):
        return block_work(None, b)

    lax.fori_loop(0, 4, one_block, 0)

    for c in sends:
        c.wait_send()
    everything = recv.at[:, pl.ds(0, n - 1)]
    pltpu.make_async_copy(everything, everything, st_recv).wait()
    pltpu.make_async_copy(everything, everything, st_send).wait()

    slot_of = {0: 0, side - 1: 1, 1: 2, 2: 3}
    low = sub < 4
    q4 = lax.rem(sub, 4)
    logs, shifts, ratios = ([None] * (2 * side) for _ in range(3))
    for g in range(side):

        def value(d):
            dx, dy = (d // 2) % side, d // (2 * side)
            a = recv[slot_of[(g - dy) % side], d]
            b = recv[slot_of[(g - dx) % side], d]
            return jnp.where(low, a, b)

        top = functools.reduce(jnp.maximum, [value(d) for d in range(n)])
        total = jnp.zeros((8, LANES), jnp.float32)
        for d in range(n):
            v = value(d)
            gap = v - top
            down = jnp.where(low, jnp.broadcast_to(gap[0:1, :], (8, LANES)), jnp.broadcast_to(gap[4:5, :], (8, LANES)))
            down = jnp.maximum(down, FLOOR)
            scaled = v * jnp.exp(down)
            moved = pltpu.roll(scaled * down, 1, 0)
            total = total + jnp.where(q4 == 3, v, scaled) + jnp.where(q4 == 2, moved, 0.0)
        for k in range(2):
            m, z, s, t = top[4 * k : 4 * k + 1], *(total[4 * k + i : 4 * k + i + 1] for i in (1, 2, 3))
            logs[k * side + g] = jnp.log(z)
            shifts[k * side + g] = t - m
            ratios[k * side + g] = s / z

    for i, parts in enumerate((shifts, logs, ratios)):
        both = jnp.concatenate(parts, axis=0)
        moved = [both] + [pltpu.roll(both, i * rows, 1) for i in range(1, side)]
        for r in range(2 * side):
            q, hx = r // 2, r % 2
            parts_ref[i, r : r + 1, :] = by_part(
                [
                    cut(moved, q, -2 * hx),
                    cut(moved, side + 2 * hx, 1 - q),
                    cut(moved, q, 1 - 2 * hx),
                    cut(moved, side + 2 * hx + 1, 3 - q),
                ]
            )
    mean_ref[0] = jnp.sum(parts_ref[0] - parts_ref[1]) / (2 * side * group)


def solution(mesh):
    n = mesh.shape["vp"]
    side = math.isqrt(n // 2)

    def local_step(hidden, target, norm_gain, head_weight):
        rows, depth = hidden.shape
        tokens = target.shape[0]
        group = rows * side
        vocab = head_weight.shape[1]
        whole = vocab // 16 * 16
        rest = head_weight.T[vocab - 16 :]
        parts, mean = pl.pallas_call(
            functools.partial(_kernel, side),
            out_shape=(
                jax.ShapeDtypeStruct((3, 2 * side, group), jnp.float32),
                jax.ShapeDtypeStruct((1,), jnp.float32),
            ),
            in_specs=[pl.BlockSpec(memory_space=pl.ANY)] * 5,
            out_specs=(
                pl.BlockSpec(memory_space=pltpu.VMEM),
                pl.BlockSpec(memory_space=pltpu.SMEM),
            ),
            scratch_shapes=[
                pltpu.VMEM((rows, depth), jnp.bfloat16),
                pltpu.VMEM((2 * side, group), jnp.int32),
                pltpu.VMEM((depth // LANES, LANES), jnp.bfloat16),
                pltpu.VMEM((whole + 16, depth), jnp.bfloat16),
                pltpu.VMEM((tokens, depth), jnp.bfloat16),
                pltpu.VMEM((2 * side, group), jnp.int32),
                pltpu.VMEM((2, 8, LANES), jnp.int32),
                *[pltpu.VMEM((8, 2 * LANES), jnp.float32)] * 4,
                pltpu.VMEM((side, 8, LANES), jnp.float32),
                pltpu.VMEM((8, LANES), jnp.float32),
                pltpu.VMEM((side, n, 8, LANES), jnp.float32),
                pltpu.VMEM((2, _chunks(vocab)[0][1], TILE), jnp.float32),
                pltpu.SemaphoreType.DMA((4,)),
                pltpu.SemaphoreType.DMA((SEGMENTS,)),
                pltpu.SemaphoreType.DMA((22,)),
                pltpu.SemaphoreType.DMA((22,)),
                pltpu.SemaphoreType.DMA,
                pltpu.SemaphoreType.DMA,
            ],
            compiler_params=pltpu.CompilerParams(
                collective_id=0, has_side_effects=True, vmem_limit_bytes=67043328
            ),
            name="score",
        )(hidden, target.reshape(2 * side, group), norm_gain.reshape(depth // LANES, LANES), rest, head_weight.T)
        shift, log_total, ratio = parts.reshape(3, tokens)
        return shift - log_total, log_total - ratio, mean

    return jax.shard_map(
        local_step,
        mesh=mesh,
        in_specs=(P(("dp", "vp"), None), P("dp"), P(None), P(None, "vp")),
        out_specs=(P("dp"), P("dp"), P("dp")),
        check_vma=False,
    )
```

```python
import functools
import math

import jax
import jax.numpy as jnp
from jax import lax
from jax.experimental import pallas as pl
from jax.experimental.pallas import tpu as pltpu
from jax.sharding import PartitionSpec as P

NORM_EPS = 1e-6
TILE = 256
LANES = 128
PIECE = 80
SEGMENTS = 3
PAIRS = 2
FLOOR = -200.0


def _chunks(vocab):
    units = -(-vocab // 16)
    count = SEGMENTS * PAIRS
    size = -(-units // (2 * count)) * 2
    out, start = [], 0
    for _ in range(count):
        both = min(size, units - start)
        for rows in (both - both // 2, both // 2):
            out.append((start * 16, min(rows * 16, vocab - start * 16)))
            start += rows
    return out


def _kernel(
    side, hid_hbm, tgt_hbm, gain_hbm, w_hbm, parts_ref, mean_ref,
    tgt, gain, w, h, ids, local_ids, ms, zs, ss, ts, stat, hold, recv, zbuf, early,
    in_sem, w_sem, s_send, s_recv, st_send, st_recv,
):
    n = 2 * side * side
    rows, depth = hid_hbm.shape
    vocab = w_hbm.shape[0]
    ktiles = depth // TILE
    group = rows * side
    me = lax.axis_index("vp")
    core = lax.rem(me, 2)
    x = lax.rem(me // 2, side)
    y = me // (2 * side)
    first = jnp.where(core == 0, x, y)
    second = jnp.where(core == 0, y, x)
    partner = me + 1 - 2 * core

    def device(p1, p2):
        return jnp.where(core == 0, (p2 * side + p1) * 2, (p1 * side + p2) * 2 + 1)

    def turn(p, by):
        return lax.rem(p + by + side, side)

    def group_row(kind, p2):
        return (kind * side + p2) * group

    half = rows // 2
    next1, prev1, far1 = turn(first, 1), turn(first, -1), turn(first, 2)
    next2, prev2, far2 = turn(second, 1), turn(second, -1), turn(second, 2)
    up1, down1 = device(next1, second), device(prev1, second)
    up2, down2 = device(first, next2), device(first, prev2)

    near = (partner, up1, down1, up2, down2)
    barrier = pltpu.get_barrier_semaphore()
    for to in near:
        pl.semaphore_signal(barrier, inc=1, device_id={"vp": to}, device_id_type=pl.DeviceIdType.MESH)

    own = pl.multiple_of(group_row(core, second) + first * rows, rows)

    small = [
        pltpu.make_async_copy(src, dst, in_sem.at[i])
        for i, (src, dst) in enumerate(((hid_hbm, h.at[pl.ds(own, rows), :]), (gain_hbm, gain), (tgt_hbm, tgt)))
    ]
    for c in small:
        c.start()
    chunks = _chunks(vocab)
    per = 2 * PAIRS

    def head_copy(i):
        cols = pl.ds(i * depth // 2, depth // 2)
        return pltpu.make_async_copy(w_hbm.at[:, cols], w.at[:, cols], w_sem.at[i])

    for i in range(2):
        head_copy(i).start(priority=1)

    small[0].wait()
    small[1].wait()
    xf = h[pl.ds(own, rows), :].astype(jnp.float32)
    inv = lax.rsqrt(jnp.mean(xf * xf, axis=-1, keepdims=True) + NORM_EPS)
    for i in range(depth // LANES):
        cols = slice(i * LANES, (i + 1) * LANES)
        part = xf[:, cols] * inv * gain[i : i + 1, :].astype(jnp.float32)
        h[pl.ds(own, rows), cols] = part.astype(jnp.bfloat16)

    def view(row, count, part):
        cols = pl.ds(0, depth) if part is None else pl.ds(part * depth // 2, depth // 2)
        return h.at[pl.ds(pl.multiple_of(row, 16), count), cols]

    def send(slot, row, count, to, part=None):
        at = view(row, count, part)
        slot += 0 if part != 1 else 22
        return pltpu.make_async_remote_copy(
            src_ref=at, dst_ref=at, send_sem=s_send.at[slot], recv_sem=s_recv.at[slot],
            device_id={"vp": to}, device_id_type=pl.DeviceIdType.MESH,
        )

    base = group_row(core, second)
    below, above, across = base + prev1 * rows, base + next1 * rows, base + far1 * rows
    pair = 2 * rows
    mine, lower, upper, opposite = (group_row(core, p) for p in (second, prev2, next2, far2))

    pl.semaphore_wait(barrier, len(near))
    sends = []

    def start(*copies):
        for c in copies:
            c.start()
        sends.extend(copies)

    def arrive(slot, count, part=None):
        send(slot, 0, count, partner, part).wait_recv()

    start(
        send(0, own, half, up1, 0),
        send(1, own + half, half, down1, 0),
        send(2, own + half, half, up1, 0),
        send(3, own, half, down1, 0),
        send(4, own, rows, partner, 0),
        send(0, own, half, up1, 1),
        send(1, own + half, half, down1, 1),
    )

    small[2].wait()
    lane1 = lax.broadcasted_iota(jnp.int32, (1, LANES), 1)
    part = lane1 // rows
    turned = [tgt[...]] + [pltpu.roll(tgt[...], i * rows, 1) for i in range(1, side)]

    def by_part(pieces):
        out = pieces[-1]
        for i in range(len(pieces) - 2, -1, -1):
            out = jnp.where(part == i, pieces[i], out)
        return out

    def cut(arrays, row, move):
        return arrays[move % side][row : row + 1]

    for g in range(side):
        ids[g : g + 1, :] = by_part([cut(turned, 2 * g + i // 2, i - i % 2 * 2) for i in range(side)])
        ids[side + g : side + g + 1, :] = by_part(
            [cut(turned, 2 * i + g // 2, i - g % 2 * 2 - 1) for i in range(side)]
        )

    arrive(0, half, 0)
    start(send(5, below, half, up1, 0))
    arrive(1, half, 0)
    start(send(6, above + half, half, down1, 0))
    start(send(2, own + half, half, up1, 1), send(3, own, half, down1, 1), send(4, own, rows, partner, 1))
    arrive(2, half, 0)
    arrive(3, half, 0)
    start(send(7, below, rows, partner, 0), send(8, above, rows, partner, 0))
    arrive(0, half, 1)
    start(send(5, below, half, up1, 1))
    arrive(1, half, 1)
    start(send(6, above + half, half, down1, 1))
    arrive(5, half, 0)
    arrive(6, half, 0)
    start(send(9, across, rows, partner, 0))
    arrive(2, half, 1)
    arrive(3, half, 1)
    start(send(7, below, rows, partner, 1), send(8, above, rows, partner, 1))
    quarter_up = jnp.where(first < 2, first, 3 - first)
    quarter_down = jnp.where(first < 2, 3 - first, first)
    start(
        send(10, mine + quarter_up * rows, rows, up2),
        send(11, mine + quarter_down * rows, rows, down2),
    )
    quarters = [
        send(9, across, rows, partner, 1),
        send(32, mine + (1 - quarter_up) * rows, rows, up2),
        send(33, mine + (5 - quarter_down) * rows, rows, down2),
    ]
    later = [send(12, mine + pair, pair, up2), send(13, mine, pair, down2)]

    forward = [send(14, lower, pair, up2), send(15, upper + pair, pair, down2)]
    share1 = [send(16, lower, pair, partner), send(17, upper + pair, pair, partner)]
    share2 = [send(18, lower + pair, pair, partner), send(19, upper, pair, partner)]
    share3 = [send(20, opposite, pair, partner), send(21, opposite + pair, pair, partner)]
    sends += quarters + later + forward + share1 + share2 + share3

    def pass_on(arrivals, copies, count=pair):
        for slot in arrivals:
            arrive(slot, count)
        for c in copies:
            c.start()

    def stat_copy(slot, count, to):
        return pltpu.make_async_remote_copy(
            src_ref=stat.at[pl.ds(slot, count)], dst_ref=recv.at[pl.ds(slot, count), me],
            send_sem=st_send, recv_sem=st_recv,
            device_id={"vp": to}, device_id_type=pl.DeviceIdType.MESH,
        )

    def spread(slot, count):
        away = [(min(dy, side - dy) + min(dx, side - dx), dy, dx, dc) for dy in range(side) for dx in range(side) for dc in range(2)]
        for _, dy, dx, dc in sorted(away, reverse=True)[:-1]:
            to = (turn(y, dy) * side + turn(x, dx)) * 2 + (core if dc == 0 else 1 - core)
            stat_copy(slot, count, to).start()

    lane = lax.broadcasted_iota(jnp.int32, (8, LANES), 1)
    sub = lax.broadcasted_iota(jnp.int32, (8, LANES), 0)

    def update(kind, row, v):
        at = pl.ds(kind * LANES, LANES)
        edge = row + v.shape[0] > vocab
        v = v.reshape(v.shape[0] // 8, 8, LANES)
        rows_at = row + 8 * lax.broadcasted_iota(jnp.int32, v.shape, 0)
        hit = local_ids[kind][None] == rows_at
        if edge:
            keep = rows_at + lax.broadcasted_iota(jnp.int32, v.shape, 1) < vocab
            v = jnp.where(keep, v, -jnp.inf)
            hit = jnp.logical_and(hit, keep)
        old = ms[:, at]
        top = jnp.maximum(old, jnp.max(v, axis=0))
        down = jnp.maximum(old - top, FLOOR)
        scale = jnp.exp(down)
        d = v - top[None]
        if edge:
            d = jnp.maximum(d, FLOOR)
        e = jnp.exp(d)
        z = zs[:, at]
        ss[:, at] = scale * (ss[:, at] + z * down) + jnp.sum(e * d, axis=0)
        zs[:, at] = scale * z + jnp.sum(e, axis=0)
        ts[:, at] += jnp.sum(jnp.where(hit, v, 0.0), axis=0)
        ms[:, at] = top

    def reset(lo, hi):
        ms[...] = jnp.full(ms.shape, -jnp.inf, jnp.float32)
        for r in (zs, ss, ts):
            r[...] = jnp.zeros(r.shape, jnp.float32)
        for kind, place in ((0, y), (1, x)):
            a = ids[pl.ds(kind * side + turn(place, lo), 1), :]
            b = ids[pl.ds(kind * side + turn(place, hi), 1), :]
            wanted = jnp.where(lane1 < pair, a, b) - me * vocab
            local_ids[kind] = jnp.broadcast_to(wanted, (8, LANES)) - sub

    def close():
        out = []
        for kind in range(2):
            at = pl.ds(kind * LANES, LANES)
            m, z = ms[:, at], zs[:, at]
            top = jnp.max(m, axis=0, keepdims=True)
            down = jnp.maximum(m - top, FLOOR)
            scale = jnp.exp(down)
            out += [
                top,
                jnp.sum(scale * z, axis=0, keepdims=True),
                jnp.sum(scale * (ss[:, at] + z * down), axis=0, keepdims=True),
                jnp.sum(ts[:, at], axis=0, keepdims=True),
            ]
        return jnp.concatenate(out, axis=0)

    def block_work(b):
        if isinstance(b, int):
            lo = hi = 0
        else:
            lo = jnp.where(b == 1, -1, jnp.where(b == 2, 1, 2))
            hi = jnp.where(b == 1, 1, jnp.where(b == 2, -1, 2))
        offsets = []
        for kind, place in ((0, y), (1, x)):
            offsets.append(pl.multiple_of(group_row(kind, turn(place, lo)), pair))
            offsets.append(pl.multiple_of(group_row(kind, turn(place, hi)) + pair, pair))

        for j in range(1, 4):
            if isinstance(b, int):
                break

            @pl.when(b == j)
            def _():
                arrive(14 + 2 * j, pair)
                arrive(15 + 2 * j, pair)
                if j == 3:
                    spread(0, 3)

        reset(lo, hi)

        def product(c, part=None):
            first_row, count = chunks[c]
            cols = slice(0, depth) if part is None else slice(part * depth // 2, (part + 1) * depth // 2)
            rhs = jnp.concatenate([h[pl.ds(o, pair), cols] for o in offsets], axis=0)
            return lax.dot_general(
                w[first_row : first_row + count, cols], rhs, (((1,), (1,)), ((), ())),
                preferred_element_type=jnp.float32,
            )

        def statistics(c, z):
            start, count = chunks[c]
            for r in range(0, count, PIECE):
                for kind in range(2):
                    last = min(r + PIECE, -(-count // 8) * 8)
                    update(kind, start + r, z[r:last, kind * LANES : (kind + 1) * LANES])

        def run(c, partial=None):
            if partial is None:
                zbuf[c % 2, : chunks[c][1]] = product(c)
            else:
                zbuf[c % 2, : chunks[c][1]] = partial[c, : chunks[c][1]] + product(c, 1)
            if c:
                statistics(c - 1, zbuf.at[(c - 1) % 2])

        if isinstance(b, int):
            head_copy(0).wait()
            for slot in (4, 7, 8, 9):
                arrive(slot, rows, 0)
            for c in range(per):
                early[c, : chunks[c][1]] = product(c, 0)
            arrive(5, half, 1)
            arrive(6, half, 1)
            for d in quarters:
                d.start()
            for c in range(per, len(chunks)):
                early[c, : chunks[c][1]] = product(c, 0)
            for slot in (4, 7, 8, 9):
                arrive(slot, rows, 1)
            for d in later:
                d.start()
            head_copy(1).wait()
            for c in range(2 * per):
                run(c, early)
            pass_on((10, 11, 32, 33), forward + share1, rows)
            for c in range(2 * per, len(chunks)):
                run(c, early)
        else:
            for c in range(len(chunks)):
                if c == len(chunks) // 2:

                    @pl.when(b == 1)
                    def _():
                        pass_on((12, 13), share2)

                    @pl.when(b == 2)
                    def _():
                        pass_on((14, 15), share3)

                run(c)
        statistics(len(chunks) - 1, zbuf.at[(len(chunks) - 1) % 2])
        finish(b)

        return 0

    def finish(b):
        p = close()

        def put(slot, v):
            stat[slot] = v
            recv[slot, me] = v

        if isinstance(b, int):
            put(0, p)
            return

        @pl.when(b == 1)
        def _():
            hold[...] = p

        @pl.when(b == 2)
        def _():
            q = hold[...]
            put(1, jnp.where(lane < pair, q, p))
            put(2, jnp.where(lane < pair, p, q))

        @pl.when(b == 3)
        def _():
            put(3, p)
            spread(3, 1)

    def one_block(b, _):
        return block_work(b)

    block_work(0)
    lax.fori_loop(1, 4, one_block, 0)

    for c in sends:
        c.wait_send()
    everything = recv.at[:, pl.ds(0, n - 1)]
    pltpu.make_async_copy(everything, everything, st_recv).wait()
    pltpu.make_async_copy(everything, everything, st_send).wait()

    slot_of = {0: 0, side - 1: 1, 1: 2, 2: 3}
    low = sub < 4
    q4 = lax.rem(sub, 4)
    logs, shifts, ratios = ([None] * (2 * side) for _ in range(3))
    for g in range(side):

        def value(d):
            dx, dy = (d // 2) % side, d // (2 * side)
            a = recv[slot_of[(g - dy) % side], d]
            b = recv[slot_of[(g - dx) % side], d]
            return jnp.where(low, a, b)

        top = functools.reduce(jnp.maximum, [value(d) for d in range(n)])
        total = jnp.zeros((8, LANES), jnp.float32)
        for d in range(n):
            v = value(d)
            gap = v - top
            down = jnp.where(low, jnp.broadcast_to(gap[0:1, :], (8, LANES)), jnp.broadcast_to(gap[4:5, :], (8, LANES)))
            down = jnp.maximum(down, FLOOR)
            scaled = v * jnp.exp(down)
            moved = pltpu.roll(scaled * down, 1, 0)
            total = total + jnp.where(q4 == 3, v, scaled) + jnp.where(q4 == 2, moved, 0.0)
        for k in range(2):
            m, z, s, t = top[4 * k : 4 * k + 1], *(total[4 * k + i : 4 * k + i + 1] for i in (1, 2, 3))
            logs[k * side + g] = jnp.log(z)
            shifts[k * side + g] = t - m
            ratios[k * side + g] = s / z

    for i, parts in enumerate((shifts, logs, ratios)):
        both = jnp.concatenate(parts, axis=0)
        moved = [both] + [pltpu.roll(both, i * rows, 1) for i in range(1, side)]
        for r in range(2 * side):
            q, hx = r // 2, r % 2
            parts_ref[i, r : r + 1, :] = by_part(
                [
                    cut(moved, q, -2 * hx),
                    cut(moved, side + 2 * hx, 1 - q),
                    cut(moved, q, 1 - 2 * hx),
                    cut(moved, side + 2 * hx + 1, 3 - q),
                ]
            )
    mean_ref[0] = jnp.sum(parts_ref[0] - parts_ref[1]) / (2 * side * group)


def solution(mesh):
    n = mesh.shape["vp"]
    side = math.isqrt(n // 2)

    def local_step(hidden, target, norm_gain, head_weight):
        rows, depth = hidden.shape
        tokens = target.shape[0]
        group = rows * side
        vocab = head_weight.shape[1]
        parts, mean = pl.pallas_call(
            functools.partial(_kernel, side),
            out_shape=(
                jax.ShapeDtypeStruct((3, 2 * side, group), jnp.float32),
                jax.ShapeDtypeStruct((1,), jnp.float32),
            ),
            in_specs=[pl.BlockSpec(memory_space=pl.ANY)] * 4,
            out_specs=(
                pl.BlockSpec(memory_space=pltpu.VMEM),
                pl.BlockSpec(memory_space=pltpu.SMEM),
            ),
            scratch_shapes=[
                pltpu.VMEM((2 * side, group), jnp.int32),
                pltpu.VMEM((depth // LANES, LANES), jnp.bfloat16),
                pltpu.VMEM((vocab, depth), jnp.bfloat16),
                pltpu.VMEM((tokens, depth), jnp.bfloat16),
                pltpu.VMEM((2 * side, group), jnp.int32),
                pltpu.VMEM((2, 8, LANES), jnp.int32),
                *[pltpu.VMEM((8, 2 * LANES), jnp.float32)] * 4,
                pltpu.VMEM((side, 8, LANES), jnp.float32),
                pltpu.VMEM((8, LANES), jnp.float32),
                pltpu.VMEM((side, n, 8, LANES), jnp.float32),
                pltpu.VMEM((2, _chunks(vocab)[0][1], TILE), jnp.float32),
                pltpu.VMEM((len(_chunks(vocab)), _chunks(vocab)[0][1], TILE), jnp.float32),
                pltpu.SemaphoreType.DMA((3,)),
                pltpu.SemaphoreType.DMA((2,)),
                pltpu.SemaphoreType.DMA((34,)),
                pltpu.SemaphoreType.DMA((34,)),
                pltpu.SemaphoreType.DMA,
                pltpu.SemaphoreType.DMA,
            ],
            compiler_params=pltpu.CompilerParams(
                collective_id=0, has_side_effects=True, vmem_limit_bytes=67043328
            ),
            name="score",
        )(hidden, target.reshape(2 * side, group), norm_gain.reshape(depth // LANES, LANES), head_weight.T)
        shift, log_total, ratio = parts.reshape(3, tokens)
        return shift - log_total, log_total - ratio, mean

    return jax.shard_map(
        local_step,
        mesh=mesh,
        in_specs=(P(("dp", "vp"), None), P("dp"), P(None), P(None, "vp")),
        out_specs=(P("dp"), P("dp"), P("dp")),
        check_vma=False,
    )
```
